8 devices in a mesh: data: 8 (over z, y, x, core).
Axes of the slice: x: 2, y: 2, z: 1, core: 2. Of those that a mesh axis runs over, the one named last changes fastest.
Arguments:
- x_tokens: bfloat16 [32768, 2048], P('data')
- dh_out: bfloat16 [32768, 2048], P('data')
- w_up: bfloat16 [2, 2048, 5632], replicated
- w_down: bfloat16 [2, 5632, 2048], replicated
- proj_up: bfloat16 [2, 2048, 512], replicated
- proj_down: bfloat16 [2, 2048, 512], replicated
- mom_up: float32 [2, 512, 5632], P(None, None, 'data')
- var_up: float32 [2, 512, 5632], P(None, None, 'data')
- mom_down: float32 [2, 5632, 512], P(None, 'data')
- var_down: float32 [2, 5632, 512], P(None, 'data')
Outputs:
- output 1: bfloat16 [2, 2048, 5632], replicated
- output 2: bfloat16 [2, 5632, 2048], replicated
- output 3: float32 [2, 512, 5632], P(None, None, 'data')
- output 4: float32 [2, 512, 5632], P(None, None, 'data')
- output 5: float32 [2, 5632, 512], P(None, 'data')
- output 6: float32 [2, 5632, 512], P(None, 'data')
All inputs are finite; a program needn't handle non-finite values.
Results may differ from the reference program's by a relative error of at most 0.00729786.
Values are sent between devices in bfloat16 or wider.
A program may use at most 1 GiB of HBM per device.

```python
import jax
import jax.numpy as jnp
from jax import lax

D = 2048
FF = 5632
RANK = 512
TOKENS = 32768
BLOCK = 2048
STEP = 4
BETA_ONE = 0.9
BETA_TWO = 0.999
EPSILON = 1e-8
LEARN_RATE = 0.02
ALPHA_SCALE = 0.25


def setup_inputs(seed: int = 0) -> dict:
    key_list = jax.random.split(jax.random.key(seed), 10)
    x_tokens = jax.random.normal(key_list[0], (TOKENS, D), jnp.float32)
    dh_out = jax.random.normal(key_list[1], (TOKENS, D), jnp.float32) * (20.0 * TOKENS ** -0.5)
    w_up = jax.random.normal(key_list[2], (2, D, FF), jnp.float32) * D ** -0.5
    w_down = jax.random.normal(key_list[3], (2, FF, D), jnp.float32) * FF ** -0.5
    proj_up = jnp.linalg.qr(jax.random.normal(key_list[4], (2, D, RANK), jnp.float32))[0]
    proj_down = jnp.linalg.qr(jax.random.normal(key_list[5], (2, D, RANK), jnp.float32))[0]
    mom_up = jax.random.normal(key_list[6], (2, RANK, FF), jnp.float32)
    var_up = jax.random.uniform(key_list[7], (2, RANK, FF), jnp.float32, 0.05, 0.15)
    mom_down = jax.random.normal(key_list[8], (2, FF, RANK), jnp.float32)
    var_down = jax.random.uniform(key_list[9], (2, FF, RANK), jnp.float32, 0.05, 0.15)
    return {
        'x_tokens': x_tokens.astype(jnp.bfloat16),
        'dh_out': dh_out.astype(jnp.bfloat16),
        'w_up': w_up.astype(jnp.bfloat16),
        'w_down': w_down.astype(jnp.bfloat16),
        'proj_up': proj_up.astype(jnp.bfloat16),
        'proj_down': proj_down.astype(jnp.bfloat16),
        'mom_up': mom_up,
        'var_up': var_up,
        'mom_down': mom_down,
        'var_down': var_down,
    }


def block_grads(x_rows, dh_rows, w_up, w_down, proj_up, proj_down):
    hidden = [x_rows]
    act_list = []
    pull_list = []
    for layer_idx in range(2):
        pre_act = jnp.dot(hidden[layer_idx], w_up[layer_idx], preferred_element_type=jnp.float32)
        gelu_val, gelu_pull = jax.vjp(jax.nn.gelu, pre_act)
        act_val = gelu_val.astype(jnp.bfloat16)
        down_out = jnp.dot(act_val, w_down[layer_idx], preferred_element_type=jnp.float32)
        hidden.append((hidden[layer_idx].astype(jnp.float32) + down_out).astype(jnp.bfloat16))
        act_list.append(act_val)
        pull_list.append(gelu_pull)
    grad_rows = dh_rows
    up_parts = [None, None]
    down_parts = [None, None]
    for layer_idx in (1, 0):
        v_proj = jnp.dot(grad_rows, proj_down[layer_idx], preferred_element_type=jnp.float32).astype(jnp.bfloat16)
        down_parts[layer_idx] = jnp.dot(act_list[layer_idx].T, v_proj, preferred_element_type=jnp.float32)
        d_act = jnp.dot(grad_rows, w_down[layer_idx].T, preferred_element_type=jnp.float32)
        d_pre = pull_list[layer_idx](d_act)[0].astype(jnp.bfloat16)
        u_proj = jnp.dot(hidden[layer_idx], proj_up[layer_idx], preferred_element_type=jnp.float32).astype(jnp.bfloat16)
        up_parts[layer_idx] = jnp.dot(u_proj.T, d_pre, preferred_element_type=jnp.float32)
        if layer_idx > 0:
            back_term = jnp.dot(d_pre, w_up[layer_idx].T, preferred_element_type=jnp.float32)
            grad_rows = (grad_rows.astype(jnp.float32) + back_term).astype(jnp.bfloat16)
    return jnp.stack(up_parts), jnp.stack(down_parts)


def adam_step(moment, variance, grad_red):
    new_mom = BETA_ONE * moment + (1.0 - BETA_ONE) * grad_red
    new_var = BETA_TWO * variance + (1.0 - BETA_TWO) * grad_red * grad_red
    bias_one = 1.0 - BETA_ONE ** STEP
    bias_two = 1.0 - BETA_TWO ** STEP
    direction = (new_mom / bias_one) / (jnp.sqrt(new_var / bias_two) + EPSILON)
    return new_mom, new_var, direction.astype(jnp.bfloat16)


def reference(x_tokens, dh_out, w_up, w_down, proj_up, proj_down, mom_up, var_up, mom_down, var_down):
    x_blocks = x_tokens.reshape(TOKENS // BLOCK, BLOCK, D)
    dh_blocks = dh_out.reshape(TOKENS // BLOCK, BLOCK, D)

    def scan_body(carry_acc, block_pair):
        part_up, part_down = block_grads(block_pair[0], block_pair[1], w_up, w_down, proj_up, proj_down)
        return (carry_acc[0] + part_up, carry_acc[1] + part_down), None

    zero_init = (jnp.zeros((2, RANK, FF), jnp.float32), jnp.zeros((2, FF, RANK), jnp.float32))
    scan_out = lax.scan(scan_body, zero_init, (x_blocks, dh_blocks))
    red_up, red_down = scan_out[0]
    new_mom_up, new_var_up, dir_up = adam_step(mom_up, var_up, red_up)
    new_mom_down, new_var_down, dir_down = adam_step(mom_down, var_down, red_down)
    delta_up = jnp.einsum('ldr,lrf->ldf', proj_up.astype(jnp.float32), dir_up.astype(jnp.float32))
    delta_down = jnp.einsum('lfr,ldr->lfd', dir_down.astype(jnp.float32), proj_down.astype(jnp.float32))
    new_w_up = (w_up.astype(jnp.float32) - (LEARN_RATE * ALPHA_SCALE) * delta_up).astype(jnp.bfloat16)
    new_w_down = (w_down.astype(jnp.float32) - (LEARN_RATE * ALPHA_SCALE) * delta_down).astype(jnp.bfloat16)
    return (new_w_up, new_w_down, new_mom_up, new_var_up, new_mom_down, new_var_down)
```

```python
import jax
import jax.numpy as jnp
from jax import lax
from jax.experimental import pallas as pl
from jax.experimental.pallas import tpu as pltpu
from jax.sharding import PartitionSpec as P


BETA_ONE = 0.9
BETA_TWO = 0.999
EPSILON = 1e-8
STEP = 4
LEARN_RATE = 0.02
ALPHA_SCALE = 0.25
GELU_C = 0.7978845608028654
GELU_A = 0.044715
VMEM_BYTES = 67_000_000
BF16 = jnp.bfloat16
F32 = jnp.float32


def dot_nn(lhs, rhs):
    return jnp.dot(lhs, rhs, preferred_element_type=F32)


def dot_tn(lhs, rhs):
    return lax.dot_general(lhs, rhs, (((0,), (0,)), ((), ())), preferred_element_type=F32)


def dot_nt(lhs, rhs):
    return lax.dot_general(lhs, rhs, (((1,), (1,)), ((), ())), preferred_element_type=F32)


def gelu_parts(z):
    sq = z * z
    s = 0.5 * jnp.tanh(z * (GELU_C + (GELU_C * GELU_A) * sq)) + 0.5
    g = z * s
    d = s + g * (1.0 - s) * (2.0 * GELU_C + (6.0 * GELU_C * GELU_A) * sq)
    return g, d


def call(body, grid, in_specs, out_specs, out_shape, flops, aliases=None):
    return pl.pallas_call(
        body, grid=grid, in_specs=in_specs, out_specs=out_specs, out_shape=out_shape,
        input_output_aliases=aliases or {},
        cost_estimate=pl.CostEstimate(flops=flops, bytes_accessed=flops // 500, transcendentals=0),
        compiler_params=pltpu.CompilerParams(vmem_limit_bytes=VMEM_BYTES))


def layer_one(h, dh, w_up, w_down, proj_up, proj_down):
    rows, d = h.shape
    ff = w_up.shape[2]
    rank = proj_up.shape[2]
    bm, bn = 1024, 512

    def body(h_ref, dh_ref, up_ref, down_ref, p_ref, q_ref, act_ref, dz_ref, u_ref, v_ref):
        @pl.when(pl.program_id(1) == 0)
        def _():
            u_ref[...] = dot_nn(h_ref[...], p_ref[0]).astype(BF16)
            v_ref[...] = dot_nn(dh_ref[...], q_ref[0]).astype(BF16)

        z = dot_nn(h_ref[...], up_ref[0])
        da = dot_nt(dh_ref[...], down_ref[0])
        g, dg = gelu_parts(z)
        act_ref[...] = g.astype(BF16)
        dz_ref[...] = (dg * da).astype(BF16)

    return call(
        body, (rows // bm, ff // bn),
        [pl.BlockSpec((bm, d), lambda i, j: (i, 0)), pl.BlockSpec((bm, d), lambda i, j: (i, 0)),
         pl.BlockSpec((1, d, bn), lambda i, j: (1, 0, j)), pl.BlockSpec((1, bn, d), lambda i, j: (1, j, 0)),
         pl.BlockSpec((1, d, rank), lambda i, j: (1, 0, 0)), pl.BlockSpec((1, d, rank), lambda i, j: (1, 0, 0))],
        [pl.BlockSpec((bm, bn), lambda i, j: (i, j))] * 2 + [pl.BlockSpec((bm, rank), lambda i, j: (i, 0))] * 2,
        [jax.ShapeDtypeStruct((rows, ff), BF16)] * 2 + [jax.ShapeDtypeStruct((rows, rank), BF16)] * 2,
        4 * rows * d * (ff + rank))(h, dh, w_up, w_down, proj_up, proj_down)


def project_pair(act, v, dz, u):
    rows, ff = act.shape
    rank = v.shape[1]
    bn = 512

    def body(act_ref, v_ref, dz_ref, u_ref, out_ref):
        out_ref[:, :rank] = dot_tn(act_ref[...], v_ref[...])
        out_ref[:, rank:] = dot_tn(dz_ref[...], u_ref[...])

    col = pl.BlockSpec((rows, bn), lambda j: (0, j))
    full = pl.BlockSpec((rows, rank), lambda j: (0, 0))
    return call(body, (ff // bn,), [col, full, col, full], pl.BlockSpec((bn, 2 * rank), lambda j: (j, 0)),
                jax.ShapeDtypeStruct((ff, 2 * rank), F32), 4 * rows * ff * rank)(act, v, dz, u)


def layer_zero_forward(x, w_up, proj_up):
    rows, d = x.shape
    ff = w_up.shape[2]
    rank = proj_up.shape[2]
    bm, bn = 2048, 512

    def body(x_ref, up_ref, p_ref, act_ref, slope_ref, u_ref):
        g, dg = gelu_parts(dot_nn(x_ref[...], up_ref[0]))
        act_ref[...] = g.astype(BF16)
        slope_ref[...] = dg

        @pl.when(pl.program_id(1) == 0)
        def _():
            u_ref[...] = dot_nn(x_ref[...], p_ref[0]).astype(BF16)

    return call(
        body, (rows // bm, ff // bn),
        [pl.BlockSpec((bm, d), lambda i, j: (i, 0)), pl.BlockSpec((1, d, bn), lambda i, j: (0, 0, j)),
         pl.BlockSpec((1, d, rank), lambda i, j: (0, 0, 0))],
        [pl.BlockSpec((bm, bn), lambda i, j: (i, j))] * 2 + [pl.BlockSpec((bm, rank), lambda i, j: (i, 0))],
        [jax.ShapeDtypeStruct((rows, ff), BF16), jax.ShapeDtypeStruct((rows, ff), F32),
         jax.ShapeDtypeStruct((rows, rank), BF16)],
        2 * rows * d * (ff + rank))(x, w_up, proj_up)


def project_one(act, v, order):
    rows, ff = act.shape
    rank = v.shape[1]
    bn = 512

    def body(act_ref, v_ref, *rest):
        rest[-1][...] = dot_tn(act_ref[...], v_ref[...])

    return call(body, (ff // bn,),
                [pl.BlockSpec((rows, bn), lambda j: (0, j)), pl.BlockSpec((rows, rank), lambda j: (0, 0))]
                + [pl.BlockSpec(memory_space=pl.ANY)] * len(order),
                pl.BlockSpec((bn, rank), lambda j: (j, 0)),
                jax.ShapeDtypeStruct((ff, rank), F32), 2 * rows * ff * rank)(act, v, *order)


def layer_zero_backward(g1, u, w_down, slope, first, count, old, order):
    rows, d = g1.shape
    ff = slope.shape[1]
    rank = u.shape[1]
    bm, bn = 2048, 512

    def body(g_ref, u_ref, down_ref, slope_ref, *rest):
        out_ref = rest[-1]
        i = pl.program_id(1)
        dz = (slope_ref[...] * dot_nt(g_ref[...], down_ref[0])).astype(BF16)
        part = dot_tn(dz, u_ref[...])

        @pl.when(i == 0)
        def _():
            out_ref[...] = part

        @pl.when(i > 0)
        def _():
            out_ref[...] += part

    extra = list(old) + list(order)
    return call(
        body, (count, rows // bm),
        [pl.BlockSpec((bm, d), lambda j, i: (i, 0)), pl.BlockSpec((bm, rank), lambda j, i: (i, 0)),
         pl.BlockSpec((1, bn, d), lambda j, i: (0, j + first, 0)),
         pl.BlockSpec((bm, bn), lambda j, i: (i, j + first))]
        + [pl.BlockSpec(memory_space=pl.ANY)] * len(extra),
        pl.BlockSpec((bn, rank), lambda j, i: (j + first, 0)),
        jax.ShapeDtypeStruct((ff, rank), F32),
        2 * rows * count * bn * (d + rank), aliases={4: 0} if old else None)(
            g1, u, w_down, slope, *extra)


def update_up(layer, w_up, proj_up, dirs, at, old, order):
    d, ff = w_up.shape[1:]
    rank = proj_up.shape[2]
    bn = 512
    scale = LEARN_RATE * ALPHA_SCALE

    def body(up_ref, p_ref, dir_ref, *rest):
        rest[-1][0] = (up_ref[0] - scale * dot_nt(p_ref[0], dir_ref[...])).astype(BF16)

    extra = list(old) + list(order)
    block = pl.BlockSpec((1, d, bn), lambda j: (layer, 0, j))
    return call(body, (ff // bn,),
                [block, pl.BlockSpec((1, d, rank), lambda j: (layer, 0, 0)),
                 pl.BlockSpec((bn, rank), lambda j: (j, at))] + [pl.BlockSpec(memory_space=pl.ANY)] * len(extra),
                block, jax.ShapeDtypeStruct(w_up.shape, BF16), 2 * d * ff * rank,
                aliases={3: 0} if old else None)(w_up, proj_up, dirs, *extra)


def update_down(layer, w_down, proj_down, dirs, at, old, order):
    ff, d = w_down.shape[1:]
    rank = proj_down.shape[2]
    bn = 512
    scale = LEARN_RATE * ALPHA_SCALE

    def body(down_ref, q_ref, dir_ref, *rest):
        rest[-1][0] = (down_ref[0] - scale * dot_nt(dir_ref[...], q_ref[0])).astype(BF16)

    extra = list(old) + list(order)
    block = pl.BlockSpec((1, bn, d), lambda j: (layer, j, 0))
    return call(body, (ff // bn,),
                [block, pl.BlockSpec((1, d, rank), lambda j: (layer, 0, 0)),
                 pl.BlockSpec((bn, rank), lambda j: (j, at))] + [pl.BlockSpec(memory_space=pl.ANY)] * len(extra),
                block, jax.ShapeDtypeStruct(w_down.shape, BF16), 2 * d * ff * rank,
                aliases={3: 0} if old else None)(w_down, proj_down, dirs, *extra)


def adam(moment, variance, grad_red):
    new_mom = BETA_ONE * moment + (1.0 - BETA_ONE) * grad_red
    new_var = BETA_TWO * variance + (1.0 - BETA_TWO) * grad_red * grad_red
    bias_one = 1.0 - BETA_ONE ** STEP
    bias_two = 1.0 - BETA_TWO ** STEP
    direction = (new_mom / bias_one) / (jnp.sqrt(new_var / bias_two) + EPSILON)
    return new_mom, new_var, direction.astype(BF16)


def solution(mesh):
    def local_step(x, dh, w_up, w_down, proj_up, proj_down, mom_up, var_up, mom_down, var_down):
        rank = proj_up.shape[2]

        def scatter(part):
            return lax.psum_scatter(part, 'data', scatter_dimension=0, tiled=True)

        def gather(part):
            return lax.all_gather(part, 'data', axis=0, tiled=True)

        a0, slope0, u0 = layer_zero_forward(x, w_up, proj_up)
        h1 = (x + dot_nn(a0, w_down[0])).astype(BF16)
        a1, dz1, u1, v1 = layer_one(h1, dh, w_up, w_down, proj_up, proj_down)
        red1 = scatter(project_pair(a1, v1, dz1, u1))
        g1 = (dh + dot_nt(dz1, w_up[1])).astype(BF16)
        v0 = dot_nn(g1, proj_down[0]).astype(BF16)

        down1 = adam(mom_down[1], var_down[1], red1[:, :rank])
        up1 = adam(mom_up[1].T, var_up[1].T, red1[:, rank:])
        dir1 = jnp.concatenate([down1[2], up1[2]], axis=1)
        dirs1 = gather(dir1)

        down0 = adam(mom_down[0], var_down[0], scatter(project_one(a0, v0, (dir1,))))
        dirs_down0 = gather(down0[2])
        blocks = w_up.shape[2] // 512
        part = layer_zero_backward(g1, u0, w_down, slope0, 0, blocks - 2, (), ())
        part = layer_zero_backward(g1, u0, w_down, slope0, blocks - 2, 2, (part,), (down0[2],))
        up0 = adam(mom_up[0].T, var_up[0].T, scatter(part))
        dirs_up0 = gather(up0[2])

        new_up = update_up(1, w_up, proj_up, dirs1, 1, (), (part,))
        new_down = update_down(1, w_down, proj_down, dirs1, 0, (), (part,))
        new_down = update_down(0, w_down, proj_down, dirs_down0, 0, (new_down,), ())
        new_up = update_up(0, w_up, proj_up, dirs_up0, 0, (new_up,), ())
        return (new_up, new_down, jnp.stack([up0[0].T, up1[0].T]), jnp.stack([up0[1].T, up1[1].T]),
                jnp.stack([down0[0], down1[0]]), jnp.stack([down0[1], down1[1]]))

    tok_spec = P('data', None)
    up_spec = P(None, None, 'data')
    down_spec = P(None, 'data', None)
    return jax.shard_map(
        local_step,
        mesh=mesh,
        in_specs=(tok_spec, tok_spec, P(), P(), P(), P(), up_spec, up_spec, down_spec, down_spec),
        out_specs=(P(), P(), up_spec, up_spec, down_spec, down_spec),
        check_vma=False,
    )
```

```python
import jax
import jax.numpy as jnp
from jax import lax
from jax.experimental import pallas as pl
from jax.experimental.pallas import tpu as pltpu
from jax.sharding import PartitionSpec as P


BETA_ONE = 0.9
BETA_TWO = 0.999
EPSILON = 1e-8
STEP = 4
LEARN_RATE = 0.02
ALPHA_SCALE = 0.25
GELU_C = 0.7978845608028654
GELU_A = 0.044715
VMEM_BYTES = 67_000_000
BF16 = jnp.bfloat16
F32 = jnp.float32


def dot_nn(lhs, rhs):
    return jnp.dot(lhs, rhs, preferred_element_type=F32)


def dot_tn(lhs, rhs):
    return lax.dot_general(lhs, rhs, (((0,), (0,)), ((), ())), preferred_element_type=F32)


def dot_nt(lhs, rhs):
    return lax.dot_general(lhs, rhs, (((1,), (1,)), ((), ())), preferred_element_type=F32)


def gelu_parts(z):
    sq = z * z
    s = 0.5 * jnp.tanh(z * (GELU_C + (GELU_C * GELU_A) * sq)) + 0.5
    g = z * s
    d = s + g * (1.0 - s) * (2.0 * GELU_C + (6.0 * GELU_C * GELU_A) * sq)
    return g, d


def call(body, grid, in_specs, out_specs, out_shape, flops, aliases=None):
    return pl.pallas_call(
        body, grid=grid, in_specs=in_specs, out_specs=out_specs, out_shape=out_shape,
        input_output_aliases=aliases or {},
        cost_estimate=pl.CostEstimate(flops=flops, bytes_accessed=flops // 500, transcendentals=0),
        compiler_params=pltpu.CompilerParams(vmem_limit_bytes=VMEM_BYTES))


def layer_one(h, dh, w_up, w_down, proj_up, proj_down):
    rows, d = h.shape
    ff = w_up.shape[2]
    rank = proj_up.shape[2]
    bm, bn = 1024, 512

    def body(h_ref, dh_ref, up_ref, down_ref, p_ref, q_ref, act_ref, dz_ref, u_ref, v_ref):
        @pl.when(pl.program_id(1) == 0)
        def _():
            u_ref[...] = dot_nn(h_ref[...], p_ref[0]).astype(BF16)
            v_ref[...] = dot_nn(dh_ref[...], q_ref[0]).astype(BF16)

        z = dot_nn(h_ref[...], up_ref[0])
        da = dot_nt(dh_ref[...], down_ref[0])
        g, dg = gelu_parts(z)
        act_ref[...] = g.astype(BF16)
        dz_ref[...] = (dg * da).astype(BF16)

    return call(
        body, (rows // bm, ff // bn),
        [pl.BlockSpec((bm, d), lambda i, j: (i, 0)), pl.BlockSpec((bm, d), lambda i, j: (i, 0)),
         pl.BlockSpec((1, d, bn), lambda i, j: (1, 0, j)), pl.BlockSpec((1, bn, d), lambda i, j: (1, j, 0)),
         pl.BlockSpec((1, d, rank), lambda i, j: (1, 0, 0)), pl.BlockSpec((1, d, rank), lambda i, j: (1, 0, 0))],
        [pl.BlockSpec((bm, bn), lambda i, j: (i, j))] * 2 + [pl.BlockSpec((bm, rank), lambda i, j: (i, 0))] * 2,
        [jax.ShapeDtypeStruct((rows, ff), BF16)] * 2 + [jax.ShapeDtypeStruct((rows, rank), BF16)] * 2,
        4 * rows * d * (ff + rank))(h, dh, w_up, w_down, proj_up, proj_down)


def back_to_zero(dh, dz, w_up, proj_down):
    rows, d = dh.shape
    ff = dz.shape[1]
    rank = proj_down.shape[2]
    bm, bn = 1024, 512
    last = d // bn - 1

    def body(dh_ref, dz_ref, up_ref, q_ref, g_ref, v_ref):
        n = pl.program_id(1)
        back = dot_nt(dz_ref[...], up_ref[0])
        g_ref[:, pl.ds(pl.multiple_of(n * bn, bn), bn)] = (dh_ref[...].astype(F32) + back).astype(BF16)

        @pl.when(n == last)
        def _():
            v_ref[...] = dot_nn(g_ref[...], q_ref[0]).astype(BF16)

    return call(
        body, (rows // bm, d // bn),
        [pl.BlockSpec((bm, bn), lambda i, n: (i, n)), pl.BlockSpec((bm, ff), lambda i, n: (i, 0)),
         pl.BlockSpec((1, bn, ff), lambda i, n: (1, n, 0)), pl.BlockSpec((1, d, rank), lambda i, n: (0, 0, 0))],
        [pl.BlockSpec((bm, d), lambda i, n: (i, 0)), pl.BlockSpec((bm, rank), lambda i, n: (i, 0))],
        [jax.ShapeDtypeStruct((rows, d), BF16), jax.ShapeDtypeStruct((rows, rank), BF16)],
        2 * rows * d * (ff + rank))(dh, dz, w_up, proj_down)


def layer_zero_forward(x, w_up, proj_up):
    rows, d = x.shape
    ff = w_up.shape[2]
    rank = proj_up.shape[2]
    bm, bn = 2048, 512

    def body(x_ref, up_ref, p_ref, act_ref, slope_ref, u_ref):
        g, dg = gelu_parts(dot_nn(x_ref[...], up_ref[0]))
        act_ref[...] = g.astype(BF16)
        slope_ref[...] = dg

        @pl.when(pl.program_id(1) == 0)
        def _():
            u_ref[...] = dot_nn(x_ref[...], p_ref[0]).astype(BF16)

    return call(
        body, (rows // bm, ff // bn),
        [pl.BlockSpec((bm, d), lambda i, j: (i, 0)), pl.BlockSpec((1, d, bn), lambda i, j: (0, 0, j)),
         pl.BlockSpec((1, d, rank), lambda i, j: (0, 0, 0))],
        [pl.BlockSpec((bm, bn), lambda i, j: (i, j))] * 2 + [pl.BlockSpec((bm, rank), lambda i, j: (i, 0))],
        [jax.ShapeDtypeStruct((rows, ff), BF16), jax.ShapeDtypeStruct((rows, ff), F32),
         jax.ShapeDtypeStruct((rows, rank), BF16)],
        2 * rows * d * (ff + rank))(x, w_up, proj_up)


def project_one(act, v, order):
    rows, ff = act.shape
    rank = v.shape[1]
    bn = 512

    def body(act_ref, v_ref, *rest):
        rest[-1][...] = dot_tn(act_ref[...], v_ref[...])

    return call(body, (ff // bn,),
                [pl.BlockSpec((rows, bn), lambda j: (0, j)), pl.BlockSpec((rows, rank), lambda j: (0, 0))]
                + [pl.BlockSpec(memory_space=pl.ANY)] * len(order),
                pl.BlockSpec((bn, rank), lambda j: (j, 0)),
                jax.ShapeDtypeStruct((ff, rank), F32), 2 * rows * ff * rank)(act, v, *order)


def layer_zero_backward(g1, u, w_down, slope, first, count, old, order):
    rows, d = g1.shape
    ff = slope.shape[1]
    rank = u.shape[1]
    bm, bn = 2048, 512

    def body(g_ref, u_ref, down_ref, slope_ref, *rest):
        out_ref = rest[-1]
        i = pl.program_id(1)
        dz = (slope_ref[...] * dot_nt(g_ref[...], down_ref[0])).astype(BF16)
        part = dot_tn(dz, u_ref[...])

        @pl.when(i == 0)
        def _():
            out_ref[...] = part

        @pl.when(i > 0)
        def _():
            out_ref[...] += part

    extra = list(old) + list(order)
    return call(
        body, (count, rows // bm),
        [pl.BlockSpec((bm, d), lambda j, i: (i, 0)), pl.BlockSpec((bm, rank), lambda j, i: (i, 0)),
         pl.BlockSpec((1, bn, d), lambda j, i: (0, j + first, 0)),
         pl.BlockSpec((bm, bn), lambda j, i: (i, j + first))]
        + [pl.BlockSpec(memory_space=pl.ANY)] * len(extra),
        pl.BlockSpec((bn, rank), lambda j, i: (j + first, 0)),
        jax.ShapeDtypeStruct((ff, rank), F32),
        2 * rows * count * bn * (d + rank), aliases={4: 0} if old else None)(
            g1, u, w_down, slope, *extra)


def update_up(layer, w_up, proj_up, dirs, at, old, order, bn=512):
    d, ff = w_up.shape[1:]
    rank = proj_up.shape[2]
    scale = LEARN_RATE * ALPHA_SCALE

    def body(up_ref, p_ref, dir_ref, *rest):
        rest[-1][0] = (up_ref[0] - scale * dot_nt(p_ref[0], dir_ref[...])).astype(BF16)

    extra = list(old) + list(order)
    block = pl.BlockSpec((1, d, bn), lambda j: (layer, 0, j))
    return call(body, (ff // bn,),
                [block, pl.BlockSpec((1, d, rank), lambda j: (layer, 0, 0)),
                 pl.BlockSpec((bn, rank), lambda j: (j, at))] + [pl.BlockSpec(memory_space=pl.ANY)] * len(extra),
                block, jax.ShapeDtypeStruct(w_up.shape, BF16), 2 * d * ff * rank,
                aliases={3: 0} if old else None)(w_up, proj_up, dirs, *extra)


def update_down(layer, w_down, proj_down, dirs, at, old, order):
    ff, d = w_down.shape[1:]
    rank = proj_down.shape[2]
    bn = 512
    scale = LEARN_RATE * ALPHA_SCALE

    def body(down_ref, q_ref, dir_ref, *rest):
        rest[-1][0] = (down_ref[0] - scale * dot_nt(dir_ref[...], q_ref[0])).astype(BF16)

    extra = list(old) + list(order)
    block = pl.BlockSpec((1, bn, d), lambda j: (layer, j, 0))
    return call(body, (ff // bn,),
                [block, pl.BlockSpec((1, d, rank), lambda j: (layer, 0, 0)),
                 pl.BlockSpec((bn, rank), lambda j: (j, at))] + [pl.BlockSpec(memory_space=pl.ANY)] * len(extra),
                block, jax.ShapeDtypeStruct(w_down.shape, BF16), 2 * d * ff * rank,
                aliases={3: 0} if old else None)(w_down, proj_down, dirs, *extra)


def adam(moment, variance, grad_red):
    new_mom = BETA_ONE * moment + (1.0 - BETA_ONE) * grad_red
    new_var = BETA_TWO * variance + (1.0 - BETA_TWO) * grad_red * grad_red
    bias_one = 1.0 - BETA_ONE ** STEP
    bias_two = 1.0 - BETA_TWO ** STEP
    direction = (new_mom / bias_one) / (jnp.sqrt(new_var / bias_two) + EPSILON)
    return new_mom, new_var, direction.astype(BF16)


def solution(mesh):
    def local_step(x, dh, w_up, w_down, proj_up, proj_down, mom_up, var_up, mom_down, var_down):
        def scatter(part):
            return lax.psum_scatter(part, 'data', scatter_dimension=0, tiled=True)

        def gather(part):
            return lax.all_gather(part, 'data', axis=0, tiled=True)

        a0, slope0, u0 = layer_zero_forward(x, w_up, proj_up)
        h1 = (x + dot_nn(a0, w_down[0])).astype(BF16)
        a1, dz1, u1, v1 = layer_one(h1, dh, w_up, w_down, proj_up, proj_down)
        part_down1 = project_one(a1, v1, ())
        part_up1 = project_one(dz1, u1, (part_down1,))
        g1, v0 = back_to_zero(dh, dz1, w_up, proj_down)

        down1 = adam(mom_down[1], var_down[1], scatter(part_down1))
        up1 = adam(mom_up[1].T, var_up[1].T, scatter(part_up1))
        dir1 = jnp.concatenate([down1[2], up1[2]], axis=1)
        dirs1 = gather(dir1)

        down0 = adam(mom_down[0], var_down[0], scatter(project_one(a0, v0, (dir1,))))
        dirs_down0 = gather(down0[2])
        blocks = w_up.shape[2] // 512
        part = layer_zero_backward(g1, u0, w_down, slope0, 0, blocks - 2, (), ())
        part = layer_zero_backward(g1, u0, w_down, slope0, blocks - 2, 2, (part,), (down0[2],))
        up0 = adam(mom_up[0].T, var_up[0].T, scatter(part))
        dirs_up0 = gather(up0[2])

        new_up = update_up(1, w_up, proj_up, dirs1, 1, (), (part,))
        new_down = update_down(1, w_down, proj_down, dirs1, 0, (), (part,))
        new_down = update_down(0, w_down, proj_down, dirs_down0, 0, (new_down,), ())
        new_up = update_up(0, w_up, proj_up, dirs_up0, 0, (new_up,), (), w_up.shape[2] // 4)
        return (new_up, new_down, jnp.stack([up0[0].T, up1[0].T]), jnp.stack([up0[1].T, up1[1].T]),
                jnp.stack([down0[0], down1[0]]), jnp.stack([down0[1], down1[1]]))

    tok_spec = P('data', None)
    up_spec = P(None, None, 'data')
    down_spec = P(None, 'data', None)
    return jax.shard_map(
        local_step,
        mesh=mesh,
        in_specs=(tok_spec, tok_spec, P(), P(), P(), P(), up_spec, up_spec, down_spec, down_spec),
        out_specs=(P(), P(), up_spec, up_spec, down_spec, down_spec),
        check_vma=False,
    )
```

```python
import jax
import jax.numpy as jnp
from jax import lax
from jax.experimental import pallas as pl
from jax.experimental.pallas import tpu as pltpu
from jax.sharding import PartitionSpec as P


BETA_ONE = 0.9
BETA_TWO = 0.999
EPSILON = 1e-8
STEP = 4
LEARN_RATE = 0.02
ALPHA_SCALE = 0.25
GELU_C = 0.7978845608028654
GELU_A = 0.044715
VMEM_BYTES = 67_000_000
BF16 = jnp.bfloat16
F32 = jnp.float32


def dot_nn(lhs, rhs):
    return jnp.dot(lhs, rhs, preferred_element_type=F32)


def dot_tn(lhs, rhs):
    return lax.dot_general(lhs, rhs, (((0,), (0,)), ((), ())), preferred_element_type=F32)


def dot_nt(lhs, rhs):
    return lax.dot_general(lhs, rhs, (((1,), (1,)), ((), ())), preferred_element_type=F32)


def gelu_parts(z):
    sq = z * z
    s = 0.5 * jnp.tanh(z * (GELU_C + (GELU_C * GELU_A) * sq)) + 0.5
    g = z * s
    d = s + g * (1.0 - s) * (2.0 * GELU_C + (6.0 * GELU_C * GELU_A) * sq)
    return g, d


def call(body, grid, in_specs, out_specs, out_shape, flops, aliases=None):
    return pl.pallas_call(
        body, grid=grid, in_specs=in_specs, out_specs=out_specs, out_shape=out_shape,
        input_output_aliases=aliases or {},
        cost_estimate=pl.CostEstimate(flops=flops, bytes_accessed=flops // 500, transcendentals=0),
        compiler_params=pltpu.CompilerParams(vmem_limit_bytes=VMEM_BYTES))


def layer_one(h, dh, w_up, w_down, proj_up, proj_down):
    rows, d = h.shape
    ff = w_up.shape[2]
    rank = proj_up.shape[2]
    bm, bn = 1024, 512

    def body(h_ref, dh_ref, up_ref, down_ref, p_ref, q_ref, act_ref, dz_ref, u_ref, v_ref):
        @pl.when(pl.program_id(1) == 0)
        def _():
            u_ref[...] = dot_nn(h_ref[...], p_ref[0]).astype(BF16)
            v_ref[...] = dot_nn(dh_ref[...], q_ref[0]).astype(BF16)

        z = dot_nn(h_ref[...], up_ref[0])
        da = dot_nt(dh_ref[...], down_ref[0])
        g, dg = gelu_parts(z)
        act_ref[...] = g.astype(BF16)
        dz_ref[...] = (dg * da).astype(BF16)

    return call(
        body, (rows // bm, ff // bn),
        [pl.BlockSpec((bm, d), lambda i, j: (i, 0)), pl.BlockSpec((bm, d), lambda i, j: (i, 0)),
         pl.BlockSpec((1, d, bn), lambda i, j: (1, 0, j)), pl.BlockSpec((1, bn, d), lambda i, j: (1, j, 0)),
         pl.BlockSpec((1, d, rank), lambda i, j: (1, 0, 0)), pl.BlockSpec((1, d, rank), lambda i, j: (1, 0, 0))],
        [pl.BlockSpec((bm, bn), lambda i, j: (i, j))] * 2 + [pl.BlockSpec((bm, rank), lambda i, j: (i, 0))] * 2,
        [jax.ShapeDtypeStruct((rows, ff), BF16)] * 2 + [jax.ShapeDtypeStruct((rows, rank), BF16)] * 2,
        4 * rows * d * (ff + rank))(h, dh, w_up, w_down, proj_up, proj_down)


def back_to_zero(dh, dz, w_up, proj_down):
    rows, d = dh.shape
    ff = dz.shape[1]
    rank = proj_down.shape[2]
    bm, bn = 1024, 512
    last = d // bn - 1

    def body(dh_ref, dz_ref, up_ref, q_ref, g_ref, v_ref):
        n = pl.program_id(1)
        back = dot_nt(dz_ref[...], up_ref[0])
        g_ref[:, pl.ds(pl.multiple_of(n * bn, bn), bn)] = (dh_ref[...].astype(F32) + back).astype(BF16)

        @pl.when(n == last)
        def _():
            v_ref[...] = dot_nn(g_ref[...], q_ref[0]).astype(BF16)

    return call(
        body, (rows // bm, d // bn),
        [pl.BlockSpec((bm, bn), lambda i, n: (i, n)), pl.BlockSpec((bm, ff), lambda i, n: (i, 0)),
         pl.BlockSpec((1, bn, ff), lambda i, n: (1, n, 0)), pl.BlockSpec((1, d, rank), lambda i, n: (0, 0, 0))],
        [pl.BlockSpec((bm, d), lambda i, n: (i, 0)), pl.BlockSpec((bm, rank), lambda i, n: (i, 0))],
        [jax.ShapeDtypeStruct((rows, d), BF16), jax.ShapeDtypeStruct((rows, rank), BF16)],
        2 * rows * d * (ff + rank))(dh, dz, w_up, proj_down)


def layer_zero_forward(x, w_up):
    rows, d = x.shape
    ff = w_up.shape[2]
    bm, bn = 1024, 512

    def body(x_ref, up_ref, act_ref, slope_ref):
        g, dg = gelu_parts(dot_nn(x_ref[...], up_ref[0]))
        act_ref[...] = g.astype(BF16)
        slope_ref[...] = dg

    return call(
        body, (rows // bm, ff // bn),
        [pl.BlockSpec((bm, d), lambda i, j: (i, 0)), pl.BlockSpec((1, d, bn), lambda i, j: (0, 0, j))],
        [pl.BlockSpec((bm, bn), lambda i, j: (i, j))] * 2,
        [jax.ShapeDtypeStruct((rows, ff), BF16), jax.ShapeDtypeStruct((rows, ff), F32)],
        2 * rows * d * ff)(x, w_up)


def project_rows(layer, h, proj, order):
    rows, d = h.shape
    rank = proj.shape[2]
    bm = 1024

    def body(h_ref, p_ref, *rest):
        rest[-1][...] = dot_nn(h_ref[...], p_ref[0]).astype(BF16)

    return call(body, (rows // bm,),
                [pl.BlockSpec((bm, d), lambda i: (i, 0)), pl.BlockSpec((1, d, rank), lambda i: (layer, 0, 0))]
                + [pl.BlockSpec(memory_space=pl.ANY)] * len(order),
                pl.BlockSpec((bm, rank), lambda i: (i, 0)),
                jax.ShapeDtypeStruct((rows, rank), BF16), 2 * rows * d * rank)(h, proj, *order)


def project_one(act, v, order):
    rows, ff = act.shape
    rank = v.shape[1]
    bn = 512

    def body(act_ref, v_ref, *rest):
        rest[-1][...] = dot_tn(act_ref[...], v_ref[...])

    return call(body, (ff // bn,),
                [pl.BlockSpec((rows, bn), lambda j: (0, j)), pl.BlockSpec((rows, rank), lambda j: (0, 0))]
                + [pl.BlockSpec(memory_space=pl.ANY)] * len(order),
                pl.BlockSpec((bn, rank), lambda j: (j, 0)),
                jax.ShapeDtypeStruct((ff, rank), F32), 2 * rows * ff * rank)(act, v, *order)


def layer_zero_backward(g1, u, w_down, slope, first, count, old, order):
    rows, d = g1.shape
    ff = slope.shape[1]
    rank = u.shape[1]
    bm, bn = 2048, 512

    def body(g_ref, u_ref, down_ref, slope_ref, *rest):
        out_ref = rest[-1]
        i = pl.program_id(1)
        dz = (slope_ref[...] * dot_nt(g_ref[...], down_ref[0])).astype(BF16)
        part = dot_tn(dz, u_ref[...])

        @pl.when(i == 0)
        def _():
            out_ref[...] = part

        @pl.when(i > 0)
        def _():
            out_ref[...] += part

    extra = list(old) + list(order)
    return call(
        body, (count, rows // bm),
        [pl.BlockSpec((bm, d), lambda j, i: (i, 0)), pl.BlockSpec((bm, rank), lambda j, i: (i, 0)),
         pl.BlockSpec((1, bn, d), lambda j, i: (0, j + first, 0)),
         pl.BlockSpec((bm, bn), lambda j, i: (i, j + first))]
        + [pl.BlockSpec(memory_space=pl.ANY)] * len(extra),
        pl.BlockSpec((bn, rank), lambda j, i: (j + first, 0)),
        jax.ShapeDtypeStruct((ff, rank), F32),
        2 * rows * count * bn * (d + rank), aliases={4: 0} if old else None)(
            g1, u, w_down, slope, *extra)


def update_up(layer, w_up, proj_up, dirs, at, old, order, bn=512):
    d, ff = w_up.shape[1:]
    rank = proj_up.shape[2]
    scale = LEARN_RATE * ALPHA_SCALE

    def body(up_ref, p_ref, dir_ref, *rest):
        rest[-1][0] = (up_ref[0] - scale * dot_nt(p_ref[0], dir_ref[...])).astype(BF16)

    extra = list(old) + list(order)
    block = pl.BlockSpec((1, d, bn), lambda j: (layer, 0, j))
    return call(body, (ff // bn,),
                [block, pl.BlockSpec((1, d, rank), lambda j: (layer, 0, 0)),
                 pl.BlockSpec((bn, rank), lambda j: (j, at))] + [pl.BlockSpec(memory_space=pl.ANY)] * len(extra),
                block, jax.ShapeDtypeStruct(w_up.shape, BF16), 2 * d * ff * rank,
                aliases={3: 0} if old else None)(w_up, proj_up, dirs, *extra)


def update_down(layer, w_down, proj_down, dirs, at, old, order):
    ff, d = w_down.shape[1:]
    rank = proj_down.shape[2]
    bn = 512
    scale = LEARN_RATE * ALPHA_SCALE

    def body(down_ref, q_ref, dir_ref, *rest):
        rest[-1][0] = (down_ref[0] - scale * dot_nt(dir_ref[...], q_ref[0])).astype(BF16)

    extra = list(old) + list(order)
    block = pl.BlockSpec((1, bn, d), lambda j: (layer, j, 0))
    return call(body, (ff // bn,),
                [block, pl.BlockSpec((1, d, rank), lambda j: (layer, 0, 0)),
                 pl.BlockSpec((bn, rank), lambda j: (j, at))] + [pl.BlockSpec(memory_space=pl.ANY)] * len(extra),
                block, jax.ShapeDtypeStruct(w_down.shape, BF16), 2 * d * ff * rank,
                aliases={3: 0} if old else None)(w_down, proj_down, dirs, *extra)


def adam(moment, variance, grad_red):
    new_mom = BETA_ONE * moment + (1.0 - BETA_ONE) * grad_red
    new_var = BETA_TWO * variance + (1.0 - BETA_TWO) * grad_red * grad_red
    bias_one = 1.0 - BETA_ONE ** STEP
    bias_two = 1.0 - BETA_TWO ** STEP
    direction = (new_mom / bias_one) / (jnp.sqrt(new_var / bias_two) + EPSILON)
    return new_mom, new_var, direction.astype(BF16)


def solution(mesh):
    def local_step(x, dh, w_up, w_down, proj_up, proj_down, mom_up, var_up, mom_down, var_down):
        def scatter(part):
            return lax.psum_scatter(part, 'data', scatter_dimension=0, tiled=True)

        def gather(part):
            return lax.all_gather(part, 'data', axis=0, tiled=True)

        a0, slope0 = layer_zero_forward(x, w_up)
        h1 = (x + dot_nn(a0, w_down[0])).astype(BF16)
        a1, dz1, u1, v1 = layer_one(h1, dh, w_up, w_down, proj_up, proj_down)
        part_down1 = project_one(a1, v1, ())
        part_up1 = project_one(dz1, u1, (part_down1,))
        u0 = project_rows(0, x, proj_up, (part_up1,))
        g1, v0 = back_to_zero(dh, dz1, w_up, proj_down)

        down1 = adam(mom_down[1], var_down[1], scatter(part_down1))
        up1 = adam(mom_up[1].T, var_up[1].T, scatter(part_up1))
        dir1 = jnp.concatenate([down1[2], up1[2]], axis=1)
        dirs1 = gather(dir1)

        down0 = adam(mom_down[0], var_down[0], scatter(project_one(a0, v0, (dir1,))))
        dirs_down0 = gather(down0[2])
        blocks = w_up.shape[2] // 512
        part = layer_zero_backward(g1, u0, w_down, slope0, 0, blocks - 3, (), ())
        part = layer_zero_backward(g1, u0, w_down, slope0, blocks - 3, 3, (part,), (down0[2],))
        up0 = adam(mom_up[0].T, var_up[0].T, scatter(part))
        dirs_up0 = gather(up0[2])

        new_up = update_up(1, w_up, proj_up, dirs1, 1, (), (part,))
        new_down = update_down(1, w_down, proj_down, dirs1, 0, (), (part,))
        new_down = update_down(0, w_down, proj_down, dirs_down0, 0, (new_down,), ())
        new_up = update_up(0, w_up, proj_up, dirs_up0, 0, (new_up,), (), w_up.shape[2] // 4)
        return (new_up, new_down, jnp.stack([up0[0].T, up1[0].T]), jnp.stack([up0[1].T, up1[1].T]),
                jnp.stack([down0[0], down1[0]]), jnp.stack([down0[1], down1[1]]))

    tok_spec = P('data', None)
    up_spec = P(None, None, 'data')
    down_spec = P(None, 'data', None)
    return jax.shard_map(
        local_step,
        mesh=mesh,
        in_specs=(tok_spec, tok_spec, P(), P(), P(), P(), up_spec, up_spec, down_spec, down_spec),
        out_specs=(P(), P(), up_spec, up_spec, down_spec, down_spec),
        check_vma=False,
    )
```
